32 devices in a mesh: groups: 2 (over x), patch: 16 (over z, y, core).
Axes of the slice: x: 2, y: 2, z: 4, core: 2. Of those that a mesh axis runs over, the one named last changes fastest.
Arguments:
- grid_latents: bfloat16 [32768, 512], P(('groups', 'patch')), parts along dimension 0, may hold values from -6 to 6
- mesh_latents: bfloat16 [16384, 512], P(('groups', 'patch')), parts along dimension 0, may hold values from -6 to 6
- enc_send: int32 [640, 128], P(('groups', 'patch')), parts along dimension 0, may hold values from 0 to 1023
- enc_recv: int32 [640, 128], P(('groups', 'patch')), parts along dimension 0, may hold values from 0 to 512, as said below
- neighbours: int32 [16384, 32], P(('groups', 'patch')), parts along dimension 0, may hold values from 0 to 8191, as said below
- enc_grid_w: bfloat16 [512, 512], replicated, may hold values from -0.25 to 0.25
- enc_bias: float32 [512], replicated, may hold values from -4 to 4
- enc_mesh_w: bfloat16 [512, 512], replicated, may hold values from -0.25 to 0.25
- enc_msg_w: bfloat16 [512, 512], replicated, may hold values from -0.25 to 0.25
- upd_agg_w: bfloat16 [512, 512], replicated, may hold values from -0.25 to 0.25
- upd_mesh_w: bfloat16 [512, 512], replicated, may hold values from -0.25 to 0.25
- upd_out_w: bfloat16 [512, 512], replicated, may hold values from -0.25 to 0.25
- norm_gain: float32 [512], replicated, may hold values from 0.1 to 1.9
- query_w: bfloat16 [512, 512], replicated, may hold values from -0.25 to 0.25
- key_w: bfloat16 [512, 512], replicated, may hold values from -0.25 to 0.25
- value_w: bfloat16 [512, 512], replicated, may hold values from -0.25 to 0.25
- out_w: bfloat16 [512, 512], replicated, may hold values from -0.25 to 0.25
- ffn_gain: float32 [512], replicated, may hold values from 0.1 to 1.9
- ffn_in_w: bfloat16 [512, 2048], replicated, may hold values from -0.25 to 0.25
- ffn_out_w: bfloat16 [2048, 512], replicated, may hold values from -0.125 to 0.125
Outputs:
- result: bfloat16 [16384, 512], P(('groups', 'patch')), parts along dimension 0
The draws below stay inside these ranges and needn't reach their ends.
There are 2 independent parts, one for each index of `groups`. The reference program is written for one: setup_inputs(seed, part) draws one part's arguments, and reference() takes and returns one part's arrays. A program takes and returns all parts, laid end to end along the dimension named above; an argument that names none is the same for every part. Nothing has to cross between parts.
Inputs may be any that keep to these rules, and one draw needn't show every extreme that they name: `enc_recv`: in each band's slots for one owner, the used edges come first and the rest hold 512; the first and last bands fill all their slots. `neighbours`: neighbour 0 of a node is the node itself; every neighbour's owner is within 2 patch indices of the node's owner, wrapping around.
All inputs are finite; a program needn't handle non-finite values.
Results may differ from the reference program's by a relative error of at most 0.006.
The reference program's roundings to bfloat16 on the way count: a program that leaves them out, or rounds other values in their place, can miss the bound.
Values may be sent and summed in bfloat16 or wider, within the bound.
A program may use at most 256 MiB of HBM per device.

```python
import math
import jax
import jax.numpy as jnp
from jax import lax

D = 512
HEADS = 4
FF = 2048
G_DEV = 1024
M_DEV = 512
EB = 4
EDGE_BLOCK = 128
REACH = 2
KNB = 32
GRID = 16384
MESH = 8192
BLOCKS = 320
N_PATCH = 16


def draw_enc_recv(key, part):
    capacity = EB * EDGE_BLOCK
    hop_count = 2 * REACH + 1
    devices = jnp.arange(N_PATCH, dtype=jnp.int32)
    distance = jnp.abs(2 * devices + 1 - N_PATCH)
    base_count = capacity // 2 + capacity // 2 * distance * distance // ((N_PATCH - 1) * (N_PATCH - 1))
    first_key, second_key = jax.random.split(key)
    removed = jax.random.randint(first_key, (N_PATCH, hop_count), 0, capacity // 16 + 1)
    removed = jnp.where((distance < N_PATCH - 1)[:, None], removed, 0)
    counts = base_count[:, None] - removed
    rows_drawn = jax.random.randint(second_key, (N_PATCH, hop_count, capacity), 0, M_DEV)
    slot_ids = jnp.arange(capacity, dtype=jnp.int32)
    filled = jnp.where(slot_ids[None, None, :] < counts[:, :, None], rows_drawn, M_DEV)
    return filled.astype(jnp.int32).reshape(N_PATCH * hop_count * EB, EDGE_BLOCK)


def draw_neighbours(key, part):
    node_ids = jnp.arange(MESH, dtype=jnp.int32)
    owners = node_ids // M_DEV
    first_key, second_key = jax.random.split(key)
    steps_drawn = jax.random.randint(first_key, (MESH, KNB), -REACH, REACH + 1)
    rows_drawn = jax.random.randint(second_key, (MESH, KNB), 0, M_DEV)
    others = (owners[:, None] + steps_drawn) % N_PATCH * M_DEV + rows_drawn
    leading = jnp.arange(KNB, dtype=jnp.int32)[None, :] == 0
    return jnp.where(leading, node_ids[:, None], others).astype(jnp.int32)


def place_ends(drawn, rng, smallest, high):
    spot = [jax.random.randint(jax.random.fold_in(rng, axis), (), 0, length) for axis, length in enumerate(drawn.shape)]
    main_axis = drawn.shape.index(max(drawn.shape))
    next_to = spot[:main_axis] + [(spot[main_axis] + 1) % drawn.shape[main_axis]] + spot[main_axis + 1:]
    return drawn.at[tuple(spot)].set(smallest).at[tuple(next_to)].set(high)


def block_scale(own_key, dims, cuts, smallest, high):
    level = 1.0
    for axis_at, parts in cuts:
        draws = jax.random.uniform(jax.random.fold_in(jax.random.fold_in(own_key, 6), axis_at), (parts,), jnp.float32, smallest / len(cuts), high / len(cuts))
        level = level * jnp.repeat(jnp.exp(draws), dims[axis_at] // parts).reshape((-1,) + (1,) * (len(dims) - 1 - axis_at))
    return level


def bell_draw(stream_key, dims, scale, most, shards=(), held_as=jnp.bfloat16):
    values = scale * jax.random.normal(stream_key, dims, jnp.float32)
    if shards:
        values = values * block_scale(stream_key, dims, shards, -0.22, 0.18)
    return jnp.clip(values, -most, most).astype(held_as)


def setup_inputs(seed: int = 0, part: int = 0) -> dict:
    streams_of = jax.random.split(jax.random.key(seed), 21)
    part_keys = jax.random.split(jax.random.fold_in(streams_of[20], part), 21)
    grid_latents = bell_draw(part_keys[0], (GRID, D), 1.0, 6.0, ((0, 16),))
    mesh_latents = bell_draw(part_keys[1], (MESH, D), 1.0, 6.0, ((0, 16),))
    enc_send = place_ends(jax.random.randint(part_keys[2], (BLOCKS, EDGE_BLOCK), 0, G_DEV), jax.random.fold_in(part_keys[2], 1), 0, G_DEV - 1).astype(jnp.int32)
    enc_recv = draw_enc_recv(jax.random.fold_in(jax.random.fold_in(streams_of[20], part), 71), part)
    neighbours = draw_neighbours(jax.random.fold_in(jax.random.fold_in(streams_of[20], part), 71), part)
    enc_grid_w = bell_draw(streams_of[5], (D, D), D ** -0.5, 0.25)
    enc_bias = bell_draw(streams_of[6], (D,), 1.0, 4.0, (), jnp.float32)
    enc_mesh_w = bell_draw(streams_of[7], (D, D), D ** -0.5, 0.25)
    enc_msg_w = bell_draw(streams_of[8], (D, D), D ** -0.5, 0.25)
    upd_agg_w = bell_draw(streams_of[9], (D, D), D ** -0.5, 0.25)
    upd_mesh_w = bell_draw(streams_of[10], (D, D), D ** -0.5, 0.25)
    upd_out_w = bell_draw(streams_of[11], (D, D), D ** -0.5, 0.25)
    norm_gain = jnp.clip(1.0 + 0.18 * jax.random.normal(streams_of[12], (D,), jnp.float32), 0.1, 1.9)
    query_w = bell_draw(streams_of[13], (D, D), D ** -0.5, 0.25)
    key_w = bell_draw(streams_of[14], (D, D), D ** -0.5, 0.25)
    value_w = bell_draw(streams_of[15], (D, D), D ** -0.5, 0.25)
    out_w = bell_draw(streams_of[16], (D, D), D ** -0.5, 0.25)
    ffn_gain = jnp.clip(1.0 + 0.18 * jax.random.normal(streams_of[17], (D,), jnp.float32), 0.1, 1.9)
    ffn_in_w = bell_draw(streams_of[18], (D, FF), D ** -0.5, 0.25)
    ffn_out_w = bell_draw(streams_of[19], (FF, D), FF ** -0.5, 0.125)
    return {"grid_latents": grid_latents, "mesh_latents": mesh_latents, "enc_send": enc_send, "enc_recv": enc_recv, "neighbours": neighbours, "enc_grid_w": enc_grid_w, "enc_bias": enc_bias, "enc_mesh_w": enc_mesh_w, "enc_msg_w": enc_msg_w, "upd_agg_w": upd_agg_w, "upd_mesh_w": upd_mesh_w, "upd_out_w": upd_out_w, "norm_gain": norm_gain, "query_w": query_w, "key_w": key_w, "value_w": value_w, "out_w": out_w, "ffn_gain": ffn_gain, "ffn_in_w": ffn_in_w, "ffn_out_w": ffn_out_w}


norm_eps = 1e-05
head_eps = 1e-06

def rms_scale(values, gain_vector):
    square = lax.optimization_barrier(jnp.mean(values * values, axis=-1, keepdims=True))
    return (values * lax.rsqrt(square + norm_eps) * gain_vector).astype(jnp.bfloat16)

def reference(grid_latents, mesh_latents, enc_send, enc_recv, neighbours, enc_grid_w, enc_bias, enc_mesh_w, enc_msg_w, upd_agg_w, upd_mesh_w, upd_out_w, norm_gain, query_w, key_w, value_w, out_w, ffn_gain, ffn_in_w, ffn_out_w):
    hop_count = 2 * REACH + 1
    capacity = EB * EDGE_BLOCK
    projected = (jnp.dot(grid_latents, enc_grid_w, preferred_element_type=jnp.float32) + enc_bias).astype(jnp.bfloat16)
    receiver_proj = jnp.dot(mesh_latents, enc_mesh_w, preferred_element_type=jnp.float32).astype(jnp.bfloat16)
    senders = enc_send.reshape(N_PATCH, hop_count, capacity)
    targets = enc_recv.reshape(N_PATCH, hop_count, capacity)
    devices = jnp.arange(N_PATCH, dtype=jnp.int32)[:, None, None]
    offsets = (jnp.arange(hop_count, dtype=jnp.int32) - REACH)[None, :, None]
    owners = (devices + offsets) % N_PATCH
    sender_ids = (devices * G_DEV + senders).reshape(N_PATCH, -1)
    receiver_ids = (owners * M_DEV + jnp.minimum(targets, M_DEV - 1)).reshape(N_PATCH, -1)
    segment_ids = jnp.where(targets < M_DEV, owners * M_DEV + targets, MESH).astype(jnp.int32).reshape(N_PATCH, -1)

    def add_device(summed, inputs):
        send_rows = jnp.take(projected, inputs[0], axis=0).astype(jnp.float32)
        recv_rows = jnp.take(receiver_proj, inputs[1], axis=0).astype(jnp.float32)
        active = jax.nn.silu(send_rows + recv_rows).astype(jnp.bfloat16)
        message = jnp.dot(active, enc_msg_w, preferred_element_type=jnp.float32).astype(jnp.bfloat16)
        return (summed + jax.ops.segment_sum(message.astype(jnp.float32), inputs[2], num_segments=MESH + 1), None)
    summed, _ = lax.scan(add_device, jnp.zeros((MESH + 1, D), jnp.float32), (sender_ids, receiver_ids, segment_ids))
    aggregate = summed[:MESH].astype(jnp.bfloat16)
    update = jax.nn.silu(jnp.dot(aggregate, upd_agg_w, preferred_element_type=jnp.float32) + jnp.dot(mesh_latents, upd_mesh_w, preferred_element_type=jnp.float32)).astype(jnp.bfloat16)
    encoded = mesh_latents.astype(jnp.float32) + jnp.dot(update, upd_out_w, preferred_element_type=jnp.float32)
    normed = rms_scale(encoded, norm_gain)
    queries = jnp.dot(normed, query_w, preferred_element_type=jnp.float32).astype(jnp.bfloat16)
    key_proj = jnp.dot(normed, key_w, preferred_element_type=jnp.float32).astype(jnp.bfloat16)
    values = jnp.dot(normed, value_w, preferred_element_type=jnp.float32).astype(jnp.bfloat16)
    head_size = D // HEADS

    def attend(inputs):
        block_queries, block_links = inputs
        row_count = block_queries.shape[0]
        neighbour_key_rows = jnp.take(key_proj, block_links.reshape(-1), axis=0).astype(jnp.float32).reshape(row_count, KNB, HEADS, head_size)
        neighbour_value_rows = jnp.take(values, block_links.reshape(-1), axis=0).astype(jnp.float32).reshape(row_count, KNB, HEADS, head_size)
        query_per_head = block_queries.astype(jnp.float32).reshape(row_count, HEADS, head_size)
        score_products = jnp.einsum('jou,jsou->jso', query_per_head, neighbour_key_rows)
        query_squares = jnp.einsum('tfe,tfe->tf', query_per_head, query_per_head)
        key_sq = jnp.einsum('mkhd,mkhd->mkh', neighbour_key_rows, neighbour_key_rows)
        scores = score_products * lax.rsqrt(query_squares / head_size + head_eps)[:, None, :] * lax.rsqrt(key_sq / head_size + head_eps) / math.sqrt(head_size)
        exponent = jnp.exp(scores)
        attention_weights = (exponent / lax.optimization_barrier(jnp.sum(exponent, axis=1, keepdims=True))).astype(jnp.bfloat16)
        attention_mixture = jnp.einsum('oia,oiae->oae', attention_weights.astype(jnp.float32), neighbour_value_rows)
        return attention_mixture.astype(jnp.bfloat16).reshape(row_count, D)
    attended = lax.map(attend, (queries.reshape(N_PATCH, M_DEV, D), neighbours.reshape(N_PATCH, M_DEV, KNB))).reshape(MESH, D)
    hidden = encoded + jnp.dot(attended, out_w, preferred_element_type=jnp.float32)
    normed_ffn = rms_scale(hidden, ffn_gain)
    expanded = jax.nn.silu(jnp.dot(normed_ffn, ffn_in_w, preferred_element_type=jnp.float32)).astype(jnp.bfloat16)
    return (hidden + jnp.dot(expanded, ffn_out_w, preferred_element_type=jnp.float32)).astype(jnp.bfloat16)
```

```python
import functools
import math

import jax
import jax.numpy as jnp
from jax import lax
from jax.experimental import pallas as pl
from jax.experimental.pallas import tpu as pltpu
from jax.sharding import PartitionSpec as P

HEADS = 4
REACH = 2
SLOTS = 2 * REACH + 1
LANES = 128
GROUP = 8
CHUNKS = 4

norm_eps = 1e-05
head_eps = 1e-06
BF = jnp.bfloat16
F32 = jnp.float32


def dot(a, b):
    return jnp.dot(a, b, preferred_element_type=F32)


def dot_nt(a, b):
    return lax.dot_general(a, b, (((1,), (1,)), ((), ())), preferred_element_type=F32)


def silu(v):
    return v / (1.0 + jnp.exp(-v))


def rms_scale(values, gain):
    square = jnp.mean(values * values, axis=-1, keepdims=True)
    return (values * lax.rsqrt(square + norm_eps) * gain).astype(BF)


def exchange_body(count, parts, *refs):
    arrays = len(parts)
    srcs, wins = refs[:arrays], refs[arrays : 2 * arrays]
    send, recv, local = refs[2 * arrays :]
    me = lax.axis_index("patch")
    core = me % 2
    chip_odd = (me // 2) % 2
    partner = me + 1 - 2 * core
    mate = me + 2 - 4 * chip_odd
    far = (me + 4 - 8 * chip_odd + count) % count
    far_from = (me - 4 + 8 * chip_odd + count) % count
    mate_slot = 4 - 4 * chip_odd
    far_slot = 4 * chip_odd

    barrier = pltpu.get_barrier_semaphore()
    for other in (partner, mate, far, far_from):
        pl.semaphore_signal(
            barrier, inc=1, device_id={"patch": other}, device_id_type=pl.DeviceIdType.MESH
        )
    pl.semaphore_wait(barrier, 4)

    def remote(src, dst, sem, other):
        return pltpu.make_async_remote_copy(
            src_ref=src,
            dst_ref=dst,
            send_sem=send.at[sem],
            recv_sem=recv.at[sem],
            device_id={"patch": other},
            device_id_type=pl.DeviceIdType.MESH,
        )

    pieces = []
    for a in range(arrays):
        rows = srcs[a].shape[0] // parts[a]
        for c in range(parts[a]):
            pieces.append((a, c * rows, rows))
    total = len(pieces)
    to_mate, to_partner, onward, passed, own = [], [], [], [], []
    for i, (a, r, n) in enumerate(pieces):
        copy = remote(srcs[a].at[pl.ds(r, n)], wins[a].at[far_slot, pl.ds(r, n)], i, mate)
        copy.start()
        to_mate.append(copy)
    for i, (a, r, n) in enumerate(pieces):
        copy = remote(
            srcs[a].at[pl.ds(r, n)], wins[a].at[1 + 2 * core, pl.ds(r, n)], total + i, partner
        )
        copy.start()
        to_partner.append(copy)
    for a in range(arrays):
        copy = pltpu.make_async_copy(srcs[a], wins[a].at[REACH], local.at[a])
        copy.start()
        own.append(copy)
    for i, (a, r, n) in enumerate(pieces):
        to_mate[i].wait_recv()
        copy = remote(
            wins[a].at[mate_slot, pl.ds(r, n)],
            wins[a].at[far_slot, pl.ds(r, n)],
            2 * total + i,
            far,
        )
        copy.start()
        onward.append(copy)
    for i, (a, r, n) in enumerate(pieces):
        onward[i].wait_recv()
        copy = remote(
            wins[a].at[4 - 4 * core, pl.ds(r, n)],
            wins[a].at[3 - 2 * core, pl.ds(r, n)],
            3 * total + i,
            partner,
        )
        copy.start()
        passed.append(copy)
    for copy in to_partner + passed:
        copy.wait_recv()
    for copy in to_mate + to_partner + onward + passed:
        copy.wait_send()
    for copy in own:
        copy.wait()


def exchange(count, collective_id, parts, *arrays):
    total = sum(parts)
    vmem = pl.BlockSpec(memory_space=pltpu.VMEM)
    return pl.pallas_call(
        functools.partial(exchange_body, count, parts),
        out_shape=[jax.ShapeDtypeStruct((SLOTS,) + a.shape, a.dtype) for a in arrays],
        in_specs=[vmem] * len(arrays),
        out_specs=[vmem] * len(arrays),
        scratch_shapes=[
            pltpu.SemaphoreType.DMA((4 * total,)),
            pltpu.SemaphoreType.DMA((4 * total,)),
            pltpu.SemaphoreType.DMA((len(arrays),)),
        ],
        compiler_params=pltpu.CompilerParams(collective_id=collective_id, has_side_effects=True),
        name="exchange",
    )(*arrays)


def encode_body(
    window, send_col, recv_col, recv_row, mesh, grid_w, bias, mesh_w, msg_w, agg_w, upd_w, out_w,
    gain, encoded_ref, normed_ref, table,
):
    grid_rows = window.shape[1]
    nodes = mesh.shape[0]
    edges = send_col.shape[1]
    half = edges // 2
    table[grid_rows:, :] = dot(mesh[...], mesh_w[...]).astype(BF)

    def hop(slot, summed):
        table[:grid_rows, :] = (dot(window[slot], grid_w[...]) + bias[...]).astype(BF)
        messages = []
        for e in (0, half):
            s = send_col[slot, pl.ds(e, half)]
            r = jnp.minimum(recv_col[slot, pl.ds(e, half)], nodes - 1)
            lane_g = lax.broadcasted_iota(jnp.int32, (half, grid_rows), 1)
            lane_m = lax.broadcasted_iota(jnp.int32, (half, nodes), 1)
            pick_s = jnp.where(s == lane_g, 1.0, 0.0).astype(BF)
            pick_r = jnp.where(r == lane_m, 1.0, 0.0).astype(BF)
            both = dot(pick_s, table[:grid_rows, :]) + dot(pick_r, table[grid_rows:, :])
            messages.append(dot(silu(both).astype(BF), msg_w[...]).astype(BF))
        message = jnp.concatenate(messages, axis=0)
        row = lax.broadcasted_iota(jnp.int32, (nodes, edges), 0)
        spread = jnp.where(recv_row[slot] == row, 1.0, 0.0).astype(BF)
        return summed + dot(spread, message)

    summed = lax.fori_loop(0, SLOTS, hop, jnp.zeros(mesh.shape, F32))
    aggregate = summed.astype(BF)
    update = silu(dot(aggregate, agg_w[...]) + dot(mesh[...], upd_w[...])).astype(BF)
    encoded = mesh[...].astype(F32) + dot(update, out_w[...])
    encoded_ref[...] = encoded
    normed_ref[...] = rms_scale(encoded, gain[...])


def attend_body(
    window, encoded, code, low, query_w, key_w, value_w, out_w, gain, in_w, ffn_w, result,
    counts, queries, keys, values, key_scale, attended,
):
    nodes, width = encoded.shape
    head = width // HEADS
    span = SLOTS * nodes
    tiles = span // LANES
    for slot in range(SLOTS):
        rows = pl.ds(slot * nodes, nodes)
        block = window[slot]
        keys[rows, :] = dot(block, key_w[...]).astype(BF)
        values[rows, :] = dot(block, value_w[...]).astype(BF)
    queries[...] = dot(window[REACH], query_w[...]).astype(BF)

    def count_group(g, carry):
        packed = GROUP * LANES // code.shape[2]
        left_row = lax.broadcasted_iota(jnp.int32, (tiles * GROUP, code.shape[2]), 0)
        right_row = lax.broadcasted_iota(jnp.int32, (LANES, code.shape[2]), 0)
        left = jnp.where(code[g] == left_row, 1.0, 0.0).astype(BF)
        right = jnp.where(low[g] == right_row, 1.0, 0.0).astype(BF)
        found = dot_nt(left, right)
        rows = pl.ds(pl.multiple_of(g * GROUP, GROUP), GROUP)
        for t in range(tiles):
            counts[rows, t * LANES : (t + 1) * LANES] = found[t * GROUP : (t + 1) * GROUP, :]
        return carry

    lax.fori_loop(0, nodes // GROUP, count_group, 0, unroll=2)

    for slot in range(SLOTS):
        cols = slice(slot * nodes, (slot + 1) * nodes)
        k = keys[cols, :].astype(F32)
        square = k * k
        upper = square.astype(BF)
        lower = (square - upper.astype(F32)).astype(BF)
        pick_row = lax.broadcasted_iota(jnp.int32, (GROUP, width), 0)
        pick_lane = lax.broadcasted_iota(jnp.int32, (GROUP, width), 1)
        pick = jnp.where(pick_lane // head == pick_row, 1.0, 0.0).astype(BF)
        sums = dot_nt(pick, upper) + dot_nt(pick, lower)
        key_scale[:, cols] = lax.rsqrt(sums / head + head_eps)

    tile = LANES

    def attend_tile(t, carry):
        rows = pl.ds(pl.multiple_of(t * tile, tile), tile)
        for h in range(HEADS):
            cols = slice(h * head, (h + 1) * head)
            q = queries[rows, cols]
            qf = q.astype(F32)
            q_scale = lax.rsqrt(jnp.sum(qf * qf, axis=1, keepdims=True) / head + head_eps)
            q_scale = q_scale * (1.0 / math.sqrt(head))
            scores = dot_nt(q, keys[:, cols]) * q_scale * key_scale[h : h + 1, :]
            exponent = jnp.exp(scores)
            c = counts[rows, :]
            inverse = 1.0 / jnp.sum(exponent * c, axis=1, keepdims=True)
            weight = (exponent * inverse).astype(BF).astype(F32)
            mixed = dot((weight * c).astype(BF), values[:, cols])
            attended[rows, cols] = mixed.astype(BF)
        return carry

    lax.fori_loop(0, nodes // tile, attend_tile, 0)

    hidden = encoded[...] + dot(attended[...], out_w[...])
    normed = rms_scale(hidden, gain[...])
    wide = in_w.shape[1]
    step = wide // 4
    total = hidden
    for f in range(0, wide, step):
        expanded = silu(dot(normed, in_w[:, f : f + step])).astype(BF)
        total = total + dot(expanded, ffn_w[f : f + step, :])
    result[...] = total.astype(BF)


def shards(
    grid_latents, mesh_latents, enc_send, enc_recv, neighbours, enc_grid_w, enc_bias, enc_mesh_w,
    enc_msg_w, upd_agg_w, upd_mesh_w, upd_out_w, norm_gain, query_w, key_w, value_w, out_w,
    ffn_gain, ffn_in_w, ffn_out_w,
):
    count = lax.axis_size("patch")
    nodes, width = mesh_latents.shape
    own_index = lax.axis_index("patch")
    blocks = enc_send.shape[0] // SLOTS
    edges = blocks * enc_send.shape[1]
    vmem = pl.BlockSpec(memory_space=pltpu.VMEM)
    params = pltpu.CompilerParams(vmem_limit_bytes=60 * 1024 * 1024)

    ends = jnp.concatenate([enc_send.reshape(SLOTS, edges), enc_recv.reshape(SLOTS, edges)], axis=0)
    ends = jnp.pad(ends, ((0, 16 - 2 * SLOTS), (0, 0)))
    grid_window, end_window = exchange(count, 0, (CHUNKS, 1), grid_latents, ends)
    sends = jnp.stack([end_window[s, SLOTS - 1 - s] for s in range(SLOTS)])
    recvs = jnp.stack([end_window[s, 2 * SLOTS - 1 - s] for s in range(SLOTS)])

    encoded, normed = pl.pallas_call(
        encode_body,
        out_shape=[
            jax.ShapeDtypeStruct((nodes, width), F32),
            jax.ShapeDtypeStruct((nodes, width), BF),
        ],
        in_specs=[vmem] * 13,
        out_specs=[vmem] * 2,
        scratch_shapes=[pltpu.VMEM((grid_latents.shape[0] + nodes, width), BF)],
        compiler_params=params,
        name="encode",
    )(
        grid_window, sends[:, :, None], recvs[:, :, None], recvs[:, None, :], mesh_latents,
        enc_grid_w, enc_bias[None, :], enc_mesh_w, enc_msg_w, upd_agg_w, upd_mesh_w, upd_out_w,
        norm_gain[None, :],
    )

    (window,) = exchange(count, 1, (CHUNKS,), normed)

    owners = neighbours // nodes
    position = (owners - own_index + REACH) % count * nodes + neighbours % nodes
    lane = jnp.arange(nodes, dtype=jnp.int32)[:, None] % GROUP
    packed = (nodes // GROUP, 1, GROUP * neighbours.shape[1])
    code = (position // LANES * GROUP + lane).reshape(packed)
    low = (position % LANES).reshape(packed)
    return pl.pallas_call(
        attend_body,
        out_shape=jax.ShapeDtypeStruct((nodes, width), BF),
        in_specs=[vmem] * 11,
        out_specs=vmem,
        scratch_shapes=[
            pltpu.VMEM((nodes, SLOTS * nodes), F32),
            pltpu.VMEM((nodes, width), BF),
            pltpu.VMEM((SLOTS * nodes, width), BF),
            pltpu.VMEM((SLOTS * nodes, width), BF),
            pltpu.VMEM((GROUP, SLOTS * nodes), F32),
            pltpu.VMEM((nodes, width), BF),
        ],
        compiler_params=params,
        name="attend",
    )(
        window, encoded, code, low, query_w, key_w, value_w, out_w, ffn_gain[None, :], ffn_in_w,
        ffn_out_w,
    )


def solution(mesh):
    rows = P(("groups", "patch"), None)
    in_specs = (rows,) * 5 + (P(),) * 15
    return jax.shard_map(shards, mesh=mesh, in_specs=in_specs, out_specs=rows, check_vma=False)
```

```python
import functools
import math

import jax
import jax.numpy as jnp
from jax import lax
from jax.experimental import pallas as pl
from jax.experimental.pallas import tpu as pltpu
from jax.sharding import PartitionSpec as P

HEADS = 4
REACH = 2
SLOTS = 2 * REACH + 1
LANES = 128
GROUP = 8
GRID_CHUNKS = 8
MESH_CHUNKS = 4

norm_eps = 1e-05
head_eps = 1e-06
BF = jnp.bfloat16
F32 = jnp.float32


def dot(a, b):
    return jnp.dot(a, b, preferred_element_type=F32)


def dot_nt(a, b):
    return lax.dot_general(a, b, (((1,), (1,)), ((), ())), preferred_element_type=F32)


def silu(v):
    return v / (1.0 + jnp.exp(-v))


def rms_scale(values, gain):
    square = jnp.mean(values * values, axis=-1, keepdims=True)
    return (values * lax.rsqrt(square + norm_eps) * gain).astype(BF)


class Relay:
    def __init__(self, count, parts, srcs, wins, send, recv, local):
        self.srcs, self.wins, self.send, self.recv, self.local = srcs, wins, send, recv, local
        me = lax.axis_index("patch")
        core = me % 2
        chip_odd = (me // 2) % 2
        self.core = core
        self.partner = me + 1 - 2 * core
        self.mate = me + 2 - 4 * chip_odd
        self.far = (me + 4 - 8 * chip_odd + count) % count
        self.far_from = (me - 4 + 8 * chip_odd + count) % count
        self.mate_slot = 4 - 4 * chip_odd
        self.far_slot = 4 * chip_odd
        self.partner_slot = 3 - 2 * core
        self.passed_slot = 1 + 2 * core
        self.pieces = []
        for a, part in enumerate(parts):
            rows = srcs[a].shape[0] // part
            for c in range(part):
                self.pieces.append((a, c * rows, rows))
        self.total = len(self.pieces)
        self.onward, self.passed = [], []

    def remote(self, src, dst, sem, other):
        return pltpu.make_async_remote_copy(
            src_ref=src,
            dst_ref=dst,
            send_sem=self.send.at[sem],
            recv_sem=self.recv.at[sem],
            device_id={"patch": other},
            device_id_type=pl.DeviceIdType.MESH,
        )

    def start(self):
        barrier = pltpu.get_barrier_semaphore()
        for other in (self.partner, self.mate, self.far, self.far_from):
            pl.semaphore_signal(
                barrier, inc=1, device_id={"patch": other}, device_id_type=pl.DeviceIdType.MESH
            )
        pl.semaphore_wait(barrier, 4)
        self.to_mate, self.to_partner = [], []
        for i, (a, r, n) in enumerate(self.pieces):
            src, win = self.srcs[a].at[pl.ds(r, n)], self.wins[a]
            self.to_mate.append(
                self.remote(src, win.at[self.far_slot, pl.ds(r, n)], i, self.mate)
            )
            self.to_mate[-1].start()
        for i, (a, r, n) in enumerate(self.pieces):
            src, win = self.srcs[a].at[pl.ds(r, n)], self.wins[a]
            self.to_partner.append(
                self.remote(
                    src, win.at[self.passed_slot, pl.ds(r, n)], self.total + i, self.partner
                )
            )
            self.to_partner[-1].start()

    def relay(self, i):
        a, r, n = self.pieces[i]
        win = self.wins[a]
        self.to_mate[i].wait_recv()
        self.onward.append(
            self.remote(
                win.at[self.mate_slot, pl.ds(r, n)],
                win.at[self.far_slot, pl.ds(r, n)],
                2 * self.total + i,
                self.far,
            )
        )
        self.onward[i].start()

    def hand_over(self, i):
        a, r, n = self.pieces[i]
        win = self.wins[a]
        self.onward[i].wait_recv()
        self.passed.append(
            self.remote(
                win.at[4 - 4 * self.core, pl.ds(r, n)],
                win.at[self.partner_slot, pl.ds(r, n)],
                3 * self.total + i,
                self.partner,
            )
        )
        self.passed[i].start()

    def finish(self):
        for copy in self.to_mate + self.to_partner + self.onward + self.passed:
            copy.wait_send()


def column(row):
    return jnp.transpose(jnp.broadcast_to(row, (LANES, LANES)))


def pick_matrix(row, size):
    lane = lax.broadcasted_iota(jnp.int32, (LANES, LANES), 1)
    blocks = []
    for e in range(0, row.shape[1], LANES):
        ids = column(row[:, e : e + LANES])
        blocks.append(
            jnp.concatenate(
                [jnp.where(ids == lane + t, 1.0, 0.0).astype(BF) for t in range(0, size, LANES)],
                axis=1,
            )
        )
    return jnp.concatenate(blocks, axis=0)


def encode_body(
    count, grid, ends, mesh, bias, gain, grid_w_in, mesh_w_in, msg_w_in, agg_w_in, upd_w_in,
    out_w_in, encoded_ref, normed_ref,
    window, end_window, table, node_table, summed,
    grid_w, mesh_w, msg_w, agg_w, upd_w, out_w, send, recv, local,
):
    loads = []
    pairs = (
        (grid_w_in, grid_w), (mesh_w_in, mesh_w), (msg_w_in, msg_w), (agg_w_in, agg_w),
        (upd_w_in, upd_w), (out_w_in, out_w), (ends, end_window.at[REACH]),
    )
    for i, (source, target) in enumerate(pairs):
        loads.append(pltpu.make_async_copy(source, target, local.at[i]))
        loads[-1].start()
    relay = Relay(count, (1, GRID_CHUNKS), (ends, grid), (end_window, window), send, recv, local)
    relay.start()
    for load in loads:
        load.wait()
    nodes = mesh.shape[0]
    edges = ends.shape[1]
    half = edges // 2
    rows = grid.shape[0] // GRID_CHUNKS
    node_table[...] = dot(mesh[...], mesh_w[...]).astype(BF)
    summed[...] = jnp.zeros(summed.shape, F32)

    def project(slot, block, r):
        table[slot, pl.ds(r, block.shape[0]), :] = (dot(block, grid_w[...]) + bias[...]).astype(BF)

    def hop(slot, between):
        sends = end_window[slot, pl.ds(SLOTS - 1 - slot, 1), :]
        recvs = end_window[slot, pl.ds(2 * SLOTS - 1 - slot, 1), :]
        messages = []
        for e in (0, half):
            pick_s = pick_matrix(sends[:, e : e + half], grid.shape[0])
            pick_r = pick_matrix(recvs[:, e : e + half], nodes)
            both = dot(pick_s, table[slot]) + dot(pick_r, node_table[...])
            messages.append(dot(silu(both).astype(BF), msg_w[...]).astype(BF))
            between()
        message = jnp.concatenate(messages, axis=0)
        row = lax.broadcasted_iota(jnp.int32, (nodes, edges), 0)
        spread = jnp.where(recvs == row, 1.0, 0.0).astype(BF)
        summed[...] += dot(spread, message)

    pumped = [0]

    def pump():
        i = pumped[0]
        relay.relay(i)
        if i > 0:
            r = relay.pieces[i][1]
            project(relay.mate_slot, window[relay.mate_slot, pl.ds(r, rows), :], r)
        pumped[0] += 1

    def idle():
        return None

    project(REACH, grid[...], 0)
    hop(REACH, pump)
    for copy in relay.to_partner:
        copy.wait_recv()
    project(relay.partner_slot, window[relay.partner_slot], 0)
    hop(relay.partner_slot, pump)
    while pumped[0] < relay.total:
        pump()

    handed = [0]

    def hand():
        i = handed[0]
        relay.hand_over(i)
        if i > 0:
            r = relay.pieces[i][1]
            project(relay.far_slot, window[relay.far_slot, pl.ds(r, rows), :], r)
        handed[0] += 1

    def hand_some():
        for _ in range(3):
            hand()

    hop(relay.mate_slot, hand_some)
    while handed[0] < relay.total:
        hand()
    hop(relay.far_slot, idle)
    for copy in relay.passed:
        copy.wait_recv()
    project(relay.passed_slot, window[relay.passed_slot], 0)
    hop(relay.passed_slot, idle)

    aggregate = summed[...].astype(BF)
    update = silu(dot(aggregate, agg_w[...]) + dot(mesh[...], upd_w[...])).astype(BF)
    encoded = mesh[...].astype(F32) + dot(update, out_w[...])
    encoded_ref[...] = encoded
    normed_ref[...] = rms_scale(encoded, gain[...])
    relay.finish()


def attend_body(
    count, normed_in, encoded, code, low, gain, query_w_in, key_w_in, value_w_in, out_w_in, in_w_in,
    ffn_w_in, result,
    window, counts, queries, keys, values, key_scale, attended,
    query_w, key_w, value_w, out_w, in_w, ffn_w, send, recv, local,
):
    nodes, width = encoded.shape
    head = width // HEADS
    span = SLOTS * nodes
    tiles = span // LANES
    loads = []
    pairs = (
        (query_w_in, query_w), (key_w_in, key_w), (value_w_in, value_w), (out_w_in, out_w),
        (in_w_in, in_w), (ffn_w_in, ffn_w),
    )
    for i, (source, target) in enumerate(pairs):
        loads.append(pltpu.make_async_copy(source, target, local.at[i]))
        loads[-1].start()
    relay = Relay(count, (MESH_CHUNKS,), (normed_in,), (window,), send, recv, local)
    relay.start()

    def project(slot, block):
        rows = pl.ds(pl.multiple_of(slot * nodes, nodes), nodes)
        k = dot(block, key_w[...]).astype(BF)
        keys[rows, :] = k
        values[rows, :] = dot(block, value_w[...]).astype(BF)
        wide = k.astype(F32)
        square = wide * wide
        upper = square.astype(BF)
        lower = (square - upper.astype(F32)).astype(BF)
        pick_row = lax.broadcasted_iota(jnp.int32, (GROUP, width), 0)
        pick_lane = lax.broadcasted_iota(jnp.int32, (GROUP, width), 1)
        pick = jnp.where(pick_lane // head == pick_row, 1.0, 0.0).astype(BF)
        sums = dot_nt(pick, upper) + dot_nt(pick, lower)
        key_scale[slot] = lax.rsqrt(sums / head + head_eps)

    def count_group(g, carry):
        left_row = lax.broadcasted_iota(jnp.int32, (tiles * GROUP, code.shape[2]), 0)
        right_row = lax.broadcasted_iota(jnp.int32, (LANES, code.shape[2]), 0)
        left = jnp.where(code[g] == left_row, 1.0, 0.0).astype(BF)
        right = jnp.where(low[g] == right_row, 1.0, 0.0).astype(BF)
        found = dot_nt(left, right)
        rows = pl.ds(pl.multiple_of(g * GROUP, GROUP), GROUP)
        for t in range(tiles):
            counts[rows, t * LANES : (t + 1) * LANES] = found[t * GROUP : (t + 1) * GROUP, :]
        return carry

    groups = nodes // GROUP
    for load in loads[:3]:
        load.wait()
    queries[...] = dot(normed_in[...], query_w[...]).astype(BF)
    project(REACH, normed_in[...])
    for i in range(MESH_CHUNKS):
        first, last = i * groups // MESH_CHUNKS, (i + 1) * groups // MESH_CHUNKS
        lax.fori_loop(first, last, count_group, 0, unroll=2)
        relay.relay(i)
    for copy in relay.to_partner:
        copy.wait_recv()
    project(relay.partner_slot, window[relay.partner_slot])
    project(relay.mate_slot, window[relay.mate_slot])
    for i in range(MESH_CHUNKS):
        relay.hand_over(i)
    project(relay.far_slot, window[relay.far_slot])
    for copy in relay.passed:
        copy.wait_recv()
    project(relay.passed_slot, window[relay.passed_slot])
    for load in loads[3:]:
        load.wait()

    tile = LANES
    def attend_tile(t, carry):
        rows = pl.ds(pl.multiple_of(t * tile, tile), tile)
        for h in range(HEADS):
            cols = slice(h * head, (h + 1) * head)
            q = queries[rows, cols]
            qf = q.astype(F32)
            q_scale = lax.rsqrt(jnp.sum(qf * qf, axis=1, keepdims=True) / head + head_eps)
            q_scale = q_scale * (1.0 / math.sqrt(head))
            k_scale = jnp.concatenate([key_scale[s, h : h + 1, :] for s in range(SLOTS)], axis=1)
            scores = dot_nt(q, keys[:, cols]) * q_scale * k_scale
            exponent = jnp.exp(scores)
            c = counts[rows, :]
            inverse = 1.0 / jnp.sum(exponent * c, axis=1, keepdims=True)
            weight = (exponent * inverse).astype(BF).astype(F32)
            mixed = dot((weight * c).astype(BF), values[:, cols])
            attended[rows, cols] = mixed.astype(BF)
        return carry

    lax.fori_loop(0, nodes // tile, attend_tile, 0)

    hidden = encoded[...] + dot(attended[...], out_w[...])
    normed = rms_scale(hidden, gain[...])
    wide = in_w.shape[1]
    step = wide // 4
    total = hidden
    for f in range(0, wide, step):
        expanded = silu(dot(normed, in_w[:, f : f + step])).astype(BF)
        total = total + dot(expanded, ffn_w[f : f + step, :])
    result[...] = total.astype(BF)
    relay.finish()


def shards(
    grid_latents, mesh_latents, enc_send, enc_recv, neighbours, enc_grid_w, enc_bias, enc_mesh_w,
    enc_msg_w, upd_agg_w, upd_mesh_w, upd_out_w, norm_gain, query_w, key_w, value_w, out_w,
    ffn_gain, ffn_in_w, ffn_out_w,
):
    count = lax.axis_size("patch")
    nodes, width = mesh_latents.shape
    own_index = lax.axis_index("patch")
    blocks = enc_send.shape[0] // SLOTS
    edges = blocks * enc_send.shape[1]
    vmem = pl.BlockSpec(memory_space=pltpu.VMEM)
    hbm = pl.BlockSpec(memory_space=pl.ANY)

    def like(a):
        return pltpu.VMEM(a.shape, a.dtype)

    def dma(n):
        return pltpu.SemaphoreType.DMA((n,))

    def params(collective_id):
        return pltpu.CompilerParams(
            vmem_limit_bytes=60 * 1024 * 1024, collective_id=collective_id, has_side_effects=True
        )

    ends = jnp.concatenate([enc_send.reshape(SLOTS, edges), enc_recv.reshape(SLOTS, edges)], axis=0)
    ends = jnp.pad(ends, ((0, 16 - 2 * SLOTS), (0, 0)))
    weights = (enc_grid_w, enc_mesh_w, enc_msg_w, upd_agg_w, upd_mesh_w, upd_out_w)
    grid_rows = grid_latents.shape[0]
    pieces = 4 * (1 + GRID_CHUNKS)
    encoded, normed = pl.pallas_call(
        functools.partial(encode_body, count),
        out_shape=[
            jax.ShapeDtypeStruct((nodes, width), F32),
            jax.ShapeDtypeStruct((nodes, width), BF),
        ],
        in_specs=[vmem] * 5 + [hbm] * 6,
        out_specs=[vmem] * 2,
        scratch_shapes=[
            pltpu.VMEM((SLOTS, grid_rows, width), BF),
            pltpu.VMEM((SLOTS,) + ends.shape, jnp.int32),
            pltpu.VMEM((SLOTS, grid_rows, width), BF),
            pltpu.VMEM((nodes, width), BF),
            pltpu.VMEM((nodes, width), F32),
        ]
        + [like(w) for w in weights]
        + [dma(pieces), dma(pieces), dma(7)],
        compiler_params=params(0),
        name="encode",
    )(grid_latents, ends, mesh_latents, enc_bias[None, :], norm_gain[None, :], *weights)

    owners = neighbours // nodes
    position = (owners - own_index + REACH) % count * nodes + neighbours % nodes
    lane = jnp.arange(nodes, dtype=jnp.int32)[:, None] % GROUP
    packed = (nodes // GROUP, 1, GROUP * neighbours.shape[1])
    code = (position // LANES * GROUP + lane).reshape(packed)
    low = (position % LANES).reshape(packed)
    weights = (query_w, key_w, value_w, out_w, ffn_in_w, ffn_out_w)
    pieces = 4 * MESH_CHUNKS
    return pl.pallas_call(
        functools.partial(attend_body, count),
        out_shape=jax.ShapeDtypeStruct((nodes, width), BF),
        in_specs=[vmem] * 5 + [hbm] * 6,
        out_specs=vmem,
        scratch_shapes=[
            pltpu.VMEM((SLOTS, nodes, width), BF),
            pltpu.VMEM((nodes, SLOTS * nodes), F32),
            pltpu.VMEM((nodes, width), BF),
            pltpu.VMEM((SLOTS * nodes, width), BF),
            pltpu.VMEM((SLOTS * nodes, width), BF),
            pltpu.VMEM((SLOTS, GROUP, nodes), F32),
            pltpu.VMEM((nodes, width), BF),
        ]
        + [like(w) for w in weights]
        + [dma(pieces), dma(pieces), dma(6)],
        compiler_params=params(1),
        name="attend",
    )(normed, encoded, code, low, ffn_gain[None, :], *weights)


def solution(mesh):
    rows = P(("groups", "patch"), None)
    in_specs = (rows,) * 5 + (P(),) * 15
    return jax.shard_map(shards, mesh=mesh, in_specs=in_specs, out_specs=rows, check_vma=False)
```
